32 devices in a mesh: col: 8 (over y, x, core), row: 4 (over z).
Axes of the slice: x: 2, y: 2, z: 4, core: 2. Of those that a mesh axis runs over, the one named last changes fastest.
Arguments:
- features: bfloat16 [65536, 2048], P(('col', 'row')), may hold values from -6 to 6
- leaf_in: bfloat16 [65536, 128], P(('col', 'row')), may hold values from -0.1875 to 0.1875
- mix_in: bfloat16 [3, 64, 128, 256], P(None, ('col', 'row')), may hold values from -0.375 to 0.375
- mix_out: bfloat16 [3, 64, 128, 256], P(None, 'col'), may hold values from -0.375 to 0.375
- leaf_out: bfloat16 [65536, 128], P('col'), may hold values from -0.5 to 0.5
Outputs:
- result: bfloat16 [65536, 2048], P(('col', 'row'))
The draws below stay inside these ranges and needn't reach their ends.
All inputs are finite; a program needn't handle non-finite values.
Results may differ from the reference program's by a relative error of at most 0.023.
Values may be sent and summed in bfloat16 or wider, within the bound.
No kernel may reach another device: no remote copies, remote signals or barrier semaphores. Data moves between devices by JAX's collectives and lax.ppermute only.
A program may use at most 128 MiB of HBM per device.

```python
import jax
import jax.numpy as jnp
from jax import lax

RANK = 128
LEAF_SIZE = 1024
RIGHT_SIDES = 2048
LEVELS_IN = 3
LEVELS_OUT = 3
LEAVES = 64
ORDER = 65536


def block_levels(own_key, shape, split, smallest, largest):
    gain = 1.0
    for axis_at, blocks in split:
        heights = jax.random.uniform(jax.random.fold_in(jax.random.fold_in(own_key, 6), axis_at), (blocks,), jnp.float32, smallest / len(split), largest / len(split))
        gain = gain * jnp.repeat(jnp.exp(heights), shape[axis_at] // blocks).reshape((-1,) + (1,) * (len(shape) - 1 - axis_at))
    return gain


def scatter_about(stream_key, shape, scale, bound, shards=(), kind=jnp.bfloat16):
    drawn = scale * jax.random.normal(stream_key, shape, jnp.float32)
    if shards:
        drawn = drawn * block_levels(stream_key, shape, shards, -0.22, 0.18)
    return jnp.clip(drawn, -bound, bound).astype(kind)


def setup_inputs(seed: int = 0) -> dict:
    key_of = jax.random.split(jax.random.key(seed), 6)
    return {
        "features": scatter_about(key_of[0], (ORDER, RIGHT_SIDES), 1.0, 6.0, ((0, 32),)),
        "leaf_in": scatter_about(key_of[1], (ORDER, RANK), LEAF_SIZE ** -0.5, 0.1875, ((0, 32),)),
        "mix_in": scatter_about(key_of[2], (LEVELS_IN, LEAVES, RANK, 2 * RANK), (2 * RANK) ** -0.5, 0.375, ((1, 32),)),
        "mix_out": scatter_about(key_of[3], (LEVELS_OUT, LEAVES, RANK, 2 * RANK), (2 * RANK) ** -0.5, 0.375, ((1, 8),)),
        "leaf_out": scatter_about(key_of[4], (ORDER, RANK), RANK ** -0.5, 0.5, ((0, 8),)),
    }


def partner_of(coeffs, level_bit):
    total_blocks = coeffs.shape[0]
    shaped = coeffs.reshape((total_blocks // (2 << level_bit), 2, 1 << level_bit) + coeffs.shape[1:])
    return jnp.flip(shaped, 1).reshape(coeffs.shape)


def forward_mix(weights, coeffs, level_bit):
    stacked = jnp.concatenate([coeffs, partner_of(coeffs, level_bit)], axis=1).astype(jnp.float32)
    return jnp.einsum('bkj,bjr->bkr', weights.astype(jnp.float32), stacked).astype(jnp.bfloat16)


def backward_mix(weights, gradient, level_bit):
    wide_weights = weights.astype(jnp.float32)
    wide_grad = gradient.astype(jnp.float32)
    direct = jnp.einsum('bjk,bjr->bkr', wide_weights[:, :, :RANK], wide_grad)
    crossed = jnp.einsum('bjk,bjr->bkr', wide_weights[:, :, RANK:], wide_grad).astype(jnp.bfloat16)
    return (direct + partner_of(crossed, level_bit).astype(jnp.float32)).astype(jnp.bfloat16)


def project(pieces):
    return jnp.dot(pieces[0].T, pieces[1], preferred_element_type=jnp.float32).astype(jnp.bfloat16)


def round_trip(pieces):
    images = jnp.dot(pieces[0], pieces[1], preferred_element_type=jnp.float32).astype(jnp.bfloat16)
    return jnp.dot(pieces[0].T, images, preferred_element_type=jnp.float32).astype(jnp.bfloat16)


def expand(pieces):
    return jnp.dot(pieces[0], pieces[1], preferred_element_type=jnp.float32).astype(jnp.bfloat16)


def reference(features, leaf_in, mix_in, mix_out, leaf_out):
    feature_blocks = features.reshape(LEAVES, LEAF_SIZE, RIGHT_SIDES)
    leaf_rows = leaf_in.reshape(LEAVES, LEAF_SIZE, RANK)
    out_rows = leaf_out.reshape(LEAVES, LEAF_SIZE, RANK)
    coeffs = lax.map(project, (leaf_rows, feature_blocks))
    for level_index in range(LEVELS_IN):
        coeffs = forward_mix(mix_in[level_index], coeffs, LEVELS_OUT + level_index)
    for level_index in range(LEVELS_OUT):
        coeffs = forward_mix(mix_out[level_index], coeffs, level_index)
    gradient = lax.map(round_trip, (out_rows, coeffs))
    for level_index in reversed(range(LEVELS_OUT)):
        gradient = backward_mix(mix_out[level_index], gradient, level_index)
    for level_index in reversed(range(LEVELS_IN)):
        gradient = backward_mix(mix_in[level_index], gradient, LEVELS_OUT + level_index)
    result = lax.map(expand, (leaf_rows, gradient))
    return result.reshape(ORDER, RIGHT_SIDES)
```

```python
import functools

import jax
import jax.numpy as jnp
from jax import lax
from jax.experimental import pallas as pl
from jax.experimental.pallas import tpu as pltpu
from jax.sharding import PartitionSpec as P

LEAF_SIZE = 1024


def swapped(block, axis, distance):
    count = lax.axis_size(axis)
    return lax.ppermute(block, axis, [(i, i ^ distance) for i in range(count)])


def project_kernel(place_ref, leaf_ref, features_ref, out_ref):
    out_ref[0] = lax.dot_general(
        leaf_ref[...], features_ref[...], (((0,), (0,)), ((), ())), preferred_element_type=jnp.float32
    ).astype(jnp.bfloat16)


def project(place, leaf_in, features, width):
    rank = leaf_in.shape[1]
    blocks = features.shape[0] // LEAF_SIZE
    flops = 2 * features.shape[0] * rank * width
    return pl.pallas_call(
        project_kernel,
        grid_spec=pltpu.PrefetchScalarGridSpec(
            num_scalar_prefetch=1,
            grid=(blocks,),
            in_specs=[
                pl.BlockSpec((LEAF_SIZE, rank), lambda b, place: (b, 0)),
                pl.BlockSpec((LEAF_SIZE, width), lambda b, place: (b, place[0])),
            ],
            out_specs=pl.BlockSpec((1, rank, width), lambda b, place: (b, 0, 0)),
        ),
        out_shape=jax.ShapeDtypeStruct((blocks, rank, width), jnp.bfloat16),
        cost_estimate=pl.CostEstimate(flops=flops, bytes_accessed=2 * features.shape[0] * width, transcendentals=0),
        name="project",
    )(place, leaf_in, features)


def expand_kernel(place_ref, leaf_ref, grad_ref, *rest):
    out_ref = rest[-1]
    out_ref[...] = jnp.dot(leaf_ref[...], grad_ref[0], preferred_element_type=jnp.float32).astype(jnp.bfloat16)


def expand(place, leaf_in, grad, sides, result):
    blocks, rank, width = grad.shape
    rows = blocks * LEAF_SIZE
    flops = 2 * rows * rank * width
    in_specs = [
        pl.BlockSpec((LEAF_SIZE, rank), lambda b, place: (b, 0)),
        pl.BlockSpec((1, rank, width), lambda b, place: (b, 0, 0)),
    ]
    operands = [place, leaf_in, grad]
    aliases = {}
    if result is not None:
        in_specs.append(pl.BlockSpec(memory_space=pl.ANY))
        operands.append(result)
        aliases = {3: 0}
    return pl.pallas_call(
        expand_kernel,
        grid_spec=pltpu.PrefetchScalarGridSpec(
            num_scalar_prefetch=1,
            grid=(blocks,),
            in_specs=in_specs,
            out_specs=pl.BlockSpec((LEAF_SIZE, width), lambda b, place: (b, place[0])),
        ),
        out_shape=jax.ShapeDtypeStruct((rows, sides), jnp.bfloat16),
        input_output_aliases=aliases,
        cost_estimate=pl.CostEstimate(flops=flops, bytes_accessed=2 * rows * width, transcendentals=0),
        name="expand",
    )(*operands)


def cluster_kernel(levels, count, shift_ref, mix_ref, leaf_ref, out_ref, first, second):
    rank = leaf_ref.shape[1]
    shift = shift_ref[0]
    for i in range(count):
        source = i ^ shift
        low = (i & ~1) * rank
        own, other = (0, rank) if i % 2 == 0 else (rank, 0)
        weights = mix_ref[0, source]
        first[pl.ds(i * rank, rank), pl.ds(low + own, rank)] = weights[:, :rank]
        first[pl.ds(i * rank, rank), pl.ds(low + other, rank)] = weights[:, rank:]
    old, new = first, second
    for level in range(1, levels):
        span = 1 << level
        for i in range(count):
            weights = mix_ref[level, i ^ shift]
            for half, partner in ((0, i), (1, i ^ span)):
                columns = pl.ds((partner & ~(span - 1)) * rank, span * rank)
                new[pl.ds(i * rank, rank), columns] = jnp.dot(
                    weights[:, half * rank : (half + 1) * rank],
                    old[pl.ds(partner * rank, rank), columns],
                    preferred_element_type=jnp.float32,
                ).astype(jnp.bfloat16)
        old, new = new, old
    for i in range(count):
        rows = pl.ds(pl.multiple_of((i ^ shift) * LEAF_SIZE, LEAF_SIZE), LEAF_SIZE)
        leaf = leaf_ref[rows, :]
        gram = lax.dot_general(
            leaf, leaf, (((0,), (0,)), ((), ())), preferred_element_type=jnp.float32
        ).astype(jnp.bfloat16)
        new[pl.ds(i * rank, rank), :] = jnp.dot(
            gram, old[pl.ds(i * rank, rank), :], preferred_element_type=jnp.float32
        ).astype(jnp.bfloat16)

    @pl.loop(0, count)
    def _(i):
        columns = pl.ds(pl.multiple_of(i * rank, rank), rank)
        out_ref[columns, :] = lax.dot_general(
            old[:, columns], new[...], (((0,), (0,)), ((), ())), preferred_element_type=jnp.float32
        ).astype(jnp.bfloat16)


def cluster_matrix(shift, mix_out, leaf_out):
    levels, count, rank, _ = mix_out.shape
    order = count * rank
    flops = 2 * order**3 + 4 * count * rank * rank * order
    return pl.pallas_call(
        functools.partial(cluster_kernel, levels, count),
        in_specs=[
            pl.BlockSpec(memory_space=pltpu.SMEM),
            pl.BlockSpec(memory_space=pltpu.VMEM),
            pl.BlockSpec(memory_space=pltpu.VMEM),
        ],
        out_specs=pl.BlockSpec(memory_space=pltpu.VMEM),
        out_shape=jax.ShapeDtypeStruct((order, order), jnp.bfloat16),
        scratch_shapes=[pltpu.VMEM((order, order), jnp.bfloat16)] * 2,
        cost_estimate=pl.CostEstimate(flops=flops, bytes_accessed=8 * order * order, transcendentals=0),
        name="cluster_matrix",
    )(shift, mix_out, leaf_out)


def apply_kernel(parts, matrix_ref, *refs):
    ins, outs = refs[:parts], refs[parts:]
    size = ins[0].shape[0]
    for o in range(parts):
        total = None
        for i in range(parts):
            term = jnp.dot(
                matrix_ref[pl.ds(o * size, size), pl.ds(i * size, size)], ins[i][...], preferred_element_type=jnp.float32
            )
            total = term if total is None else total + term
        outs[o][...] = total.astype(jnp.bfloat16)


def apply_matrix(matrix, blocks):
    parts = len(blocks)
    size, width = blocks[0].shape
    order = parts * size
    return pl.pallas_call(
        functools.partial(apply_kernel, parts),
        in_specs=[pl.BlockSpec(memory_space=pltpu.VMEM)] * (parts + 1),
        out_specs=[pl.BlockSpec(memory_space=pltpu.VMEM)] * parts,
        out_shape=[jax.ShapeDtypeStruct((size, width), jnp.bfloat16)] * parts,
        cost_estimate=pl.CostEstimate(flops=2 * order * order * width, bytes_accessed=2 * order * order, transcendentals=0),
        name="apply_matrix",
    )(matrix, *blocks)


def mixed(weights, coeffs, partner):
    rank = coeffs.shape[1]
    own = jnp.einsum("bkj,bjr->bkr", weights[:, :, :rank], coeffs, preferred_element_type=jnp.float32)
    other = jnp.einsum("bkj,bjr->bkr", weights[:, :, rank:], partner, preferred_element_type=jnp.float32)
    return (own + other).astype(jnp.bfloat16)


def returned(weights, grad, distance):
    rank = grad.shape[1]
    crossed = jnp.einsum(
        "bjk,bjr->bkr", weights[:, :, rank:], grad, preferred_element_type=jnp.float32
    ).astype(jnp.bfloat16)
    crossed = swapped(crossed, "col", distance)
    direct = jnp.einsum("bjk,bjr->bkr", weights[:, :, :rank], grad, preferred_element_type=jnp.float32)
    return (direct + crossed).astype(jnp.bfloat16)


def body(features, leaf_in, mix_in, mix_out, leaf_out):
    rank = leaf_in.shape[1]
    sides = features.shape[1]
    blocks = features.shape[0] // LEAF_SIZE
    parts = lax.axis_size("row")
    col_bits = lax.axis_size("col").bit_length() - 1
    width = sides // parts
    row = lax.axis_index("row")
    order = list(reversed(range(parts)))
    places = [jnp.reshape(row ^ step, (1,)) for step in range(parts)]

    gathered = [None] * parts
    for step in order:
        coeffs = project(places[step], leaf_in, features, width)
        for bit in range(col_bits):
            coeffs = mixed(mix_in[bit], coeffs, swapped(coeffs, "col", 1 << bit))
        coeffs = coeffs.reshape(blocks * rank, width)
        gathered[step] = swapped(coeffs, "row", step) if step else coeffs

    matrix = cluster_matrix(jnp.reshape(row * blocks, (1,)), mix_out, leaf_out)
    grads = apply_matrix(matrix, gathered)

    result = None
    for step in reversed(order):
        grad = swapped(grads[step], "row", step) if step else grads[step]
        grad = grad.reshape(blocks, rank, width)
        for bit in reversed(range(col_bits)):
            grad = returned(mix_in[bit], grad, 1 << bit)
        result = expand(places[step], leaf_in, grad, sides, result)
    return result


def solution(mesh):
    in_specs = (
        P(("col", "row"), None),
        P(("col", "row"), None),
        P(None, ("col", "row"), None, None),
        P(None, "col", None, None),
        P("col", None),
    )
    out_specs = P(("col", "row"), None)
    return jax.shard_map(body, mesh=mesh, in_specs=in_specs, out_specs=out_specs, check_vma=False)
```
